64 devices in a mesh: dp: 4 (over x, y), tp: 16 (over z, core).
Axes of the slice: x: 2, y: 2, z: 8, core: 2. Of those that a mesh axis runs over, the one named last changes fastest.
The devices are a block of a 4x4x8 slice.
Arguments:
- hidden: bfloat16 [24, 384, 6144], P('dp', 'tp'), parts along dimension 0
- lengths: int32 [24], P('dp'), parts along dimension 0
- rope_cos: float32 [24, 384, 32], P('dp'), parts along dimension 0
- rope_sin: float32 [24, 384, 32], P('dp'), parts along dimension 0
- cache_lat: bfloat16 [24, 2432, 512], P('dp'), parts along dimension 0
- cache_pe: bfloat16 [24, 2432, 64], P('dp'), parts along dimension 0
- norm_in: float32 [6144], replicated
- w_dq: bfloat16 [6144, 1536], replicated
- norm_q: float32 [1536], replicated
- w_dkv: bfloat16 [6144, 576], replicated
- norm_kv: float32 [512], replicated
- w_uq: bfloat16 [1536, 64, 192], P(None, 'tp')
- w_uk: bfloat16 [512, 64, 128], P(None, 'tp')
- w_uv: bfloat16 [512, 64, 128], P(None, 'tp')
- w_out: bfloat16 [8192, 6144], P('tp')
Outputs:
- output 1: bfloat16 [24, 384, 6144], P('dp', 'tp'), parts along dimension 0
- output 2: bfloat16 [24, 2432, 512], P('dp'), parts along dimension 0
- output 3: bfloat16 [24, 2432, 64], P('dp'), parts along dimension 0
There are 4 independent parts. The reference program is written for one: setup_inputs(seed, part) draws one part's arguments, and reference() takes and returns one part's arrays. A program takes and returns all parts, laid end to end along the dimension named above; an argument that names none is the same for every part.
All inputs are finite; a program needn't handle non-finite values.
Results may differ from the reference program's by a relative error of at most 0.0158764.
Values are sent between devices in bfloat16 or wider.
A program may use at most 768 MiB of HBM per device.

```python
import jax
import jax.numpy as jnp
from jax import lax

MODEL_DIM = 6144
NUM_HEADS = 64
Q_RANK = 1536
KV_RANK = 512
NOPE_DIM = 128
ROPE_DIM = 64
VALUE_DIM = 128
SEQ_COUNT = 6
CHUNK_LEN = 384
PREFIX_MAX = 2048
CACHE_LEN = 2432

HEAD_BLOCK = min(8, NUM_HEADS)


def rms_norm(values, gain_vec):
    inv_rms = lax.rsqrt(jnp.mean(values * values, axis=-1, keepdims=True) + 1e-6)
    return values * inv_rms * gain_vec


def apply_rope(values, cos_tab, sin_tab):
    half_dim = values.shape[-1] // 2
    lower_half = values[..., :half_dim]
    upper_half = values[..., half_dim:]
    return jnp.concatenate([lower_half * cos_tab - upper_half * sin_tab, upper_half * cos_tab + lower_half * sin_tab], axis=-1)


def write_rows(old_rows, new_rows, start_row):
    zero_col = jnp.zeros((), start_row.dtype)
    return lax.dynamic_update_slice(old_rows, new_rows.astype(old_rows.dtype), (start_row, zero_col))


def rope_tables(lengths):
    positions = (lengths[:, None] + jnp.arange(CHUNK_LEN)[None, :]).astype(jnp.float32)
    inv_freq = 10000.0 ** (-2.0 * jnp.arange(ROPE_DIM // 2).astype(jnp.float32) / ROPE_DIM)
    angles = positions[:, :, None] * inv_freq[None, None, :]
    return jnp.cos(angles), jnp.sin(angles)


def normal_draw(key_in, array_shape, std_scale):
    return jax.random.normal(key_in, array_shape, jnp.float32) * std_scale


def setup_inputs(seed: int = 0, part: int = 0) -> dict:
    base_key = jax.random.key(seed)
    part_keys = jax.random.split(jax.random.fold_in(base_key, part), 5)
    weight_keys = jax.random.split(base_key, 9)
    draw_vals = jax.random.randint(part_keys[0], (SEQ_COUNT,), PREFIX_MAX // 4, PREFIX_MAX + 1)
    top_slot = jax.random.randint(part_keys[1], (), 0, SEQ_COUNT)
    lengths = jnp.where(jnp.arange(SEQ_COUNT) == top_slot, PREFIX_MAX, draw_vals).astype(jnp.int32)
    rope_cos, rope_sin = rope_tables(lengths)
    out_scale = (NUM_HEADS * VALUE_DIM) ** -0.5 * (CACHE_LEN / 4.0) ** 0.5
    return {
        "hidden": normal_draw(part_keys[2], (SEQ_COUNT, CHUNK_LEN, MODEL_DIM), 1.0).astype(jnp.bfloat16),
        "lengths": lengths,
        "rope_cos": rope_cos,
        "rope_sin": rope_sin,
        "cache_lat": normal_draw(part_keys[3], (SEQ_COUNT, CACHE_LEN, KV_RANK), 1.0).astype(jnp.bfloat16),
        "cache_pe": normal_draw(part_keys[4], (SEQ_COUNT, CACHE_LEN, ROPE_DIM), 1.0).astype(jnp.bfloat16),
        "norm_in": jax.random.uniform(weight_keys[0], (MODEL_DIM,), jnp.float32, 0.5, 1.5),
        "w_dq": normal_draw(weight_keys[1], (MODEL_DIM, Q_RANK), MODEL_DIM ** -0.5).astype(jnp.bfloat16),
        "norm_q": jax.random.uniform(weight_keys[2], (Q_RANK,), jnp.float32, 0.5, 1.5),
        "w_dkv": normal_draw(weight_keys[3], (MODEL_DIM, KV_RANK + ROPE_DIM), MODEL_DIM ** -0.5).astype(jnp.bfloat16),
        "norm_kv": jax.random.uniform(weight_keys[4], (KV_RANK,), jnp.float32, 0.5, 1.5),
        "w_uq": normal_draw(weight_keys[5], (Q_RANK, NUM_HEADS, NOPE_DIM + ROPE_DIM), Q_RANK ** -0.5).astype(jnp.bfloat16),
        "w_uk": normal_draw(weight_keys[6], (KV_RANK, NUM_HEADS, NOPE_DIM), KV_RANK ** -0.5).astype(jnp.bfloat16),
        "w_uv": normal_draw(weight_keys[7], (KV_RANK, NUM_HEADS, VALUE_DIM), KV_RANK ** -0.5).astype(jnp.bfloat16),
        "w_out": normal_draw(weight_keys[8], (NUM_HEADS * VALUE_DIM, MODEL_DIM), out_scale).astype(jnp.bfloat16),
    }


def reference(hidden, lengths, rope_cos, rope_sin, cache_lat, cache_pe, norm_in, w_dq, norm_q, w_dkv, norm_kv, w_uq, w_uk, w_uv, w_out):
    hidden_f = hidden.astype(jnp.float32)
    normed = rms_norm(hidden_f, norm_in).astype(jnp.bfloat16).reshape(SEQ_COUNT * CHUNK_LEN, MODEL_DIM)
    q_latent = rms_norm(jnp.dot(normed, w_dq, preferred_element_type=jnp.float32), norm_q).astype(jnp.bfloat16)
    kv_proj = jnp.dot(normed, w_dkv, preferred_element_type=jnp.float32).reshape(SEQ_COUNT, CHUNK_LEN, KV_RANK + ROPE_DIM)
    new_lat = rms_norm(kv_proj[..., :KV_RANK], norm_kv).astype(jnp.bfloat16)
    new_pe = apply_rope(kv_proj[..., KV_RANK:], rope_cos, rope_sin).astype(jnp.bfloat16)
    lat_all = jax.vmap(write_rows)(cache_lat, new_lat, lengths)
    pe_all = jax.vmap(write_rows)(cache_pe, new_pe, lengths)
    q_full = jnp.einsum("nc,chd->nhd", q_latent.astype(jnp.float32), w_uq.astype(jnp.float32)).reshape(SEQ_COUNT, CHUNK_LEN, NUM_HEADS, NOPE_DIM + ROPE_DIM)
    q_nope = q_full[..., :NOPE_DIM].astype(jnp.bfloat16)
    q_pe = apply_rope(q_full[..., NOPE_DIM:], rope_cos[:, :, None, :], rope_sin[:, :, None, :]).astype(jnp.bfloat16)
    block_count = NUM_HEADS // HEAD_BLOCK
    uk_blocks = w_uk.reshape(KV_RANK, block_count, HEAD_BLOCK, NOPE_DIM).transpose(1, 0, 2, 3)
    uv_blocks = w_uv.reshape(KV_RANK, block_count, HEAD_BLOCK, VALUE_DIM).transpose(1, 0, 2, 3)
    score_scale = (NOPE_DIM + ROPE_DIM) ** -0.5
    query_pos = jnp.arange(CHUNK_LEN)[:, None]
    key_pos = jnp.arange(CACHE_LEN)[None, :]

    def one_sequence(seq_args):
        qn_seq, qp_seq, lat_seq, pe_seq, length = seq_args
        visible = key_pos < length + query_pos + 1
        qn_blocks = qn_seq.reshape(CHUNK_LEN, block_count, HEAD_BLOCK, NOPE_DIM).transpose(1, 0, 2, 3)
        qp_blocks = qp_seq.reshape(CHUNK_LEN, block_count, HEAD_BLOCK, ROPE_DIM).transpose(1, 0, 2, 3)
        lat_f = lat_seq.astype(jnp.float32)
        pe_f = pe_seq.astype(jnp.float32)

        def one_block(blk_args):
            qn_blk, qp_blk, uk_blk, uv_blk = blk_args
            keys_nope = jnp.einsum("sc,chd->shd", lat_f, uk_blk.astype(jnp.float32)).astype(jnp.bfloat16)
            values_blk = jnp.einsum("sc,chv->shv", lat_f, uv_blk.astype(jnp.float32)).astype(jnp.bfloat16)
            scores = jnp.einsum("thd,shd->hts", qn_blk.astype(jnp.float32), keys_nope.astype(jnp.float32))
            scores = scores + jnp.einsum("thr,sr->hts", qp_blk.astype(jnp.float32), pe_f)
            scores = jnp.where(visible[None], scores * score_scale, -1e30)
            attn_probs = jax.nn.softmax(scores, axis=-1).astype(jnp.bfloat16)
            return jnp.einsum("hts,shv->thv", attn_probs.astype(jnp.float32), values_blk.astype(jnp.float32)).astype(jnp.bfloat16)

        out_blocks = lax.map(one_block, (qn_blocks, qp_blocks, uk_blocks, uv_blocks))
        return out_blocks.transpose(1, 0, 2, 3).reshape(CHUNK_LEN, NUM_HEADS * VALUE_DIM)

    attn_out = lax.map(one_sequence, (q_nope, q_pe, lat_all, pe_all, lengths))
    out_proj = jnp.dot(attn_out.reshape(SEQ_COUNT * CHUNK_LEN, NUM_HEADS * VALUE_DIM), w_out, preferred_element_type=jnp.float32)
    block_out = (out_proj.reshape(SEQ_COUNT, CHUNK_LEN, MODEL_DIM) + hidden_f).astype(jnp.bfloat16)
    return (block_out, lat_all, pe_all)
```

```python
import jax
import jax.numpy as jnp
from jax import lax
from jax.sharding import PartitionSpec as P


def rms_norm(values, gain_vec):
    inv_rms = lax.rsqrt(jnp.mean(values * values, axis=-1, keepdims=True) + 1e-6)
    return values * inv_rms * gain_vec


def apply_rope(values, cos_tab, sin_tab):
    half_dim = values.shape[-1] // 2
    lower_half = values[..., :half_dim]
    upper_half = values[..., half_dim:]
    return jnp.concatenate([lower_half * cos_tab - upper_half * sin_tab, upper_half * cos_tab + lower_half * sin_tab], axis=-1)


def dot(a, b):
    return jnp.dot(a, b, preferred_element_type=jnp.float32)


def solution(mesh):
    tp_size = mesh.shape["tp"]

    def local_step(hidden, lengths, rope_cos, rope_sin, cache_lat, cache_pe, norm_in, w_dq, norm_q, w_dkv, norm_kv, w_uq, w_uk, w_uv, w_out):
        seqs, own_len, model_dim = hidden.shape
        chunk_len = own_len * tp_size
        kv_rank, heads_local, nope_dim = w_uk.shape
        value_dim = w_uv.shape[2]
        rope_dim = cache_pe.shape[2]
        cache_len = cache_lat.shape[1]
        me = lax.axis_index("tp")
        own_cos = lax.dynamic_slice_in_dim(rope_cos, me * own_len, own_len, axis=1)
        own_sin = lax.dynamic_slice_in_dim(rope_sin, me * own_len, own_len, axis=1)

        normed = rms_norm(hidden.astype(jnp.float32), norm_in).astype(jnp.bfloat16).reshape(seqs * own_len, model_dim)
        kv_proj = dot(normed, w_dkv).reshape(seqs, own_len, kv_rank + rope_dim)
        own_lat = rms_norm(kv_proj[..., :kv_rank], norm_kv).astype(jnp.bfloat16)
        own_pe = apply_rope(kv_proj[..., kv_rank:], own_cos, own_sin).astype(jnp.bfloat16)
        own_q = rms_norm(dot(normed, w_dq), norm_q).astype(jnp.bfloat16).reshape(seqs, own_len, -1)
        new_kv = lax.all_gather(jnp.concatenate([own_lat, own_pe], axis=-1), "tp", axis=1, tiled=True)
        q_latent = lax.all_gather(own_q, "tp", axis=1, tiled=True)

        lat_all, pe_all = cache_lat, cache_pe
        for b in range(seqs):
            lat_all = lax.dynamic_update_slice(lat_all, new_kv[b : b + 1, :, :kv_rank], (b, lengths[b], 0))
            pe_all = lax.dynamic_update_slice(pe_all, new_kv[b : b + 1, :, kv_rank:], (b, lengths[b], 0))

        scale = (nope_dim + rope_dim) ** -0.5
        outs = []
        for b in range(seqs):
            q_full = jnp.einsum("tq,qhd->htd", q_latent[b], w_uq, preferred_element_type=jnp.float32)
            q_nope = q_full[..., :nope_dim].astype(jnp.bfloat16)
            q_pe = apply_rope(q_full[..., nope_dim:], rope_cos[b], rope_sin[b]).astype(jnp.bfloat16)
            keys_nope = jnp.einsum("sc,chd->hsd", lat_all[b], w_uk, preferred_element_type=jnp.float32).astype(jnp.bfloat16)
            values = jnp.einsum("sc,chv->hsv", lat_all[b], w_uv, preferred_element_type=jnp.float32).astype(jnp.bfloat16)
            keys = jnp.concatenate([keys_nope, jnp.broadcast_to(pe_all[b][None], (heads_local, cache_len, rope_dim))], axis=-1)
            queries = jnp.concatenate([q_nope, q_pe], axis=-1)
            scores = jnp.einsum("htd,hsd->hts", queries, keys, preferred_element_type=jnp.float32)
            visible = jnp.arange(cache_len)[None, :] < lengths[b] + jnp.arange(chunk_len)[:, None] + 1
            scores = jnp.where(visible[None], scores * scale, -1e30)
            probs = jax.nn.softmax(scores, axis=-1).astype(jnp.bfloat16)
            attn = jnp.einsum("hts,hsv->thv", probs, values, preferred_element_type=jnp.float32).astype(jnp.bfloat16)
            head_sum = dot(attn.reshape(chunk_len, heads_local * value_dim), w_out)
            reduced = lax.psum_scatter(head_sum, "tp", scatter_dimension=0, tiled=True)
            outs.append((reduced + hidden[b].astype(jnp.float32)).astype(jnp.bfloat16))
        return jnp.stack(outs), lat_all, pe_all

    spec_tok = P("dp", "tp", None)
    spec_len = P("dp")
    spec_seq = P("dp", None, None)
    spec_vec = P(None)
    spec_mat = P(None, None)
    spec_head = P(None, "tp", None)
    spec_rows = P("tp", None)
    in_specs = (spec_tok, spec_len, spec_seq, spec_seq, spec_seq, spec_seq, spec_vec, spec_mat, spec_vec, spec_mat, spec_vec, spec_head, spec_head, spec_head, spec_rows)
    return jax.shard_map(local_step, mesh=mesh, in_specs=in_specs, out_specs=(spec_tok, spec_seq, spec_seq), check_vma=False)
```
